128 devices in a mesh: mom: 8 (over x_lo, y), en: 16 (over z, x_hi, core).
Axes of the slice: x: 4 (x_hi: 2, x_lo: 2; x = x_hi * 2 + x_lo), y: 4, z: 4, core: 2. Of those that a mesh axis runs over, the one named last changes fastest.
Arguments:
- green_blocks: float32 [24, 16, 2, 512, 512], P('mom', 'en'), may hold values from -6 to 6
- transfer_index: int32 [24, 24], P('mom'), may hold values from 0 to 8
- photon_shift: int32 [24], P('mom'), may hold values from 1 to 2
- photon_occupancy: float32 [1], replicated, may hold values from 0.3 to 3
- coupling: bfloat16 [9, 512, 512], replicated, may hold values from -0.25 to 0.25
Outputs:
- self_energy: float32 [24, 16, 2, 512, 512], P('mom', 'en')
The draws below stay inside these ranges and needn't reach their ends.
All inputs are finite; a program needn't handle non-finite values.
Results may differ from the reference program's by a relative error of at most 0.0057.
Values may be sent and summed in bfloat16 or wider, within the bound.
A program may use at most 192 MiB of HBM per device.

```python
import math
import jax
import jax.numpy as jnp
from jax import lax

NORB = 512
MOMENTA = 24
ENERGIES = 16
QC = 9


def set_ends(drawn, own_key, low, top_value):
    place = [jax.random.randint(jax.random.fold_in(own_key, axis), (), 0, length) for axis, length in enumerate(drawn.shape)]
    main_axis = drawn.shape.index(max(drawn.shape))
    next_to = place[:main_axis] + [(place[main_axis] + 1) % drawn.shape[main_axis]] + place[main_axis + 1:]
    return drawn.at[tuple(place)].set(low).at[tuple(next_to)].set(top_value)


def block_levels(own_key, extent, pieces, smallest, high):
    factor_of = 1.0
    for dim, blocks in pieces:
        heights = jax.random.uniform(jax.random.fold_in(jax.random.fold_in(own_key, 6), dim), (blocks,), jnp.float32, smallest / len(pieces), high / len(pieces))
        factor_of = factor_of * jnp.repeat(jnp.exp(heights), extent[dim] // blocks).reshape((-1,) + (1,) * (len(extent) - 1 - dim))
    return factor_of


def bell_draw(rng, shape, deviation, most, cuts=(), kind=jnp.bfloat16):
    values = deviation * jax.random.normal(rng, shape, jnp.float32)
    if cuts:
        values = values * block_levels(rng, shape, cuts, -0.22, 0.18)
    return jnp.clip(values, -most, most).astype(kind)


def setup_inputs(seed: int = 0) -> dict:
    arg_keys = jax.random.split(jax.random.key(seed), 6)
    green_blocks = bell_draw(arg_keys[0], (MOMENTA, ENERGIES, 2, NORB, NORB), 1.0, 6.0, ((0, 8), (1, 16)), jnp.float32)
    transfer_index = set_ends(jax.random.randint(arg_keys[1], (MOMENTA, MOMENTA), 0, QC), jax.random.fold_in(arg_keys[1], 1), 0, QC - 1).astype(jnp.int32)
    photon_shift = set_ends(jax.random.randint(arg_keys[2], (MOMENTA,), 1, 3), jax.random.fold_in(arg_keys[2], 1), 1, 2).astype(jnp.int32)
    photon_occupancy = jnp.clip(jnp.exp(jax.random.uniform(arg_keys[3], (1,), jnp.float32, math.log(0.3), math.log(3.0))), 0.3, 3.0)
    coupling = bell_draw(arg_keys[4], (QC, NORB, NORB), NORB ** -0.5, 0.25)
    return dict(green_blocks=green_blocks, transfer_index=transfer_index, photon_shift=photon_shift, photon_occupancy=photon_occupancy, coupling=coupling)


def reference(green_blocks, transfer_index, photon_shift, photon_occupancy, coupling):
    rounded = green_blocks.astype(jnp.bfloat16)
    padded = jnp.pad(rounded, ((0, 0), (2, 2), (0, 0), (0, 0), (0, 0)))
    near_mask = (photon_shift == 1)[:, None, None, None, None]
    below_rim = jnp.where(near_mask, padded[:, 1:1 + ENERGIES], padded[:, 0:ENERGIES])
    above_rim = jnp.where(near_mask, padded[:, 3:3 + ENERGIES], padded[:, 4:4 + ENERGIES])
    occupy = photon_occupancy[0]
    selector = (transfer_index[:, None, :] == jnp.arange(QC, dtype=jnp.int32)[None, :, None]).astype(jnp.float32)
    selector = selector.reshape(MOMENTA * QC, MOMENTA)
    weights = coupling.astype(jnp.float32)

    def one_energy(pair):
        below, above = pair
        mixed = (occupy * below.astype(jnp.float32) + (occupy + 1.0) * above.astype(jnp.float32)).astype(jnp.bfloat16)
        bins = jnp.dot(selector, mixed.astype(jnp.float32).reshape(MOMENTA, -1), precision=lax.Precision.HIGHEST)
        bins = bins.astype(jnp.bfloat16).reshape(MOMENTA, QC, 2, NORB, NORB)
        left = jnp.einsum('qxy,kqcyz->kqcxz', weights, bins.astype(jnp.float32), precision=lax.Precision.HIGHEST)
        left = left.astype(jnp.bfloat16)
        result = jnp.einsum('kqcxy,qzy->kcxz', left.astype(jnp.float32), weights, precision=lax.Precision.HIGHEST)
        return result / MOMENTA

    output = lax.map(one_energy, (jnp.moveaxis(below_rim, 1, 0), jnp.moveaxis(above_rim, 1, 0)))
    return jnp.moveaxis(output, 0, 1)
```

```python
import functools

import jax
import jax.numpy as jnp
from jax import lax
from jax.experimental import pallas as pl
from jax.experimental.pallas import tpu as pltpu
from jax.sharding import PartitionSpec as P

MESH = pl.DeviceIdType.MESH
BF = jnp.bfloat16
F32 = jnp.float32

NX, NY, NZ = 2, 4, 4
ROWS = 32
SUB = 2
RELAYED = ("b1", "b3", "a1", "a3", "r1", "r3", "z", "do", "ds", "yp", "ym", "qp", "qm")


def kernel(n, nq, own_k, perm, ends, weight, green, coupling, out,
           stage, a, own, far, rp, rc, po, ps, whole, cmat, cst, block, prefix, bins, right, obf, orecv,
           load_sem, cload_sem, send_sem, recv_sem, osend_sem, orecv_sem, store_sem):
    chunks = n // ROWS
    half = ROWS // 2
    height = ROWS * SUB
    blocks = chunks // SUB
    pair_k = 2 * own_k
    every_k = NY * pair_k
    mom, en = lax.axis_index("mom"), lax.axis_index("en")
    xl, y = mom // NY, mom % NY
    z, xh, core = en // 4, (en // 2) % 2, en % 2
    part = xl
    mine, other = xl * own_k, (1 - xl) * own_k
    up, down = (y + 1) % NY, (y + NY - 1) % NY

    def place(axl, ay, az, axh, acore):
        return (axl * NY + ay, (az * 2 + axh) * 2 + acore)

    pair = place(1 - xl, y, z, xh, core)
    cross = place(1 - xl, y, z, 1 - xh, core)
    z_to = place(xl, y, (z + 1 + 2 * xh) % NZ, xh, core)
    z_from = place(xl, y, (z + 3 + 2 * xh) % NZ, xh, core)
    twin = place(xl, y, z, xh, 1 - core)
    y_up = place(xl, up, z, xh, core)
    y_down = place(xl, down, z, xh, core)
    side = (core + xh) % 2

    kinds = {name: i for i, name in enumerate(RELAYED)}

    def remote(name, r, src, dst, device):
        i = kinds[name]
        return pltpu.make_async_remote_copy(
            src_ref=src, dst_ref=dst, send_sem=send_sem.at[i], recv_sem=recv_sem.at[i, r],
            device_id=device, device_id_type=MESH)

    def first(r):
        return own.at[r, pl.ds(mine, own_k), pl.ds(0, half)]

    def second(r):
        return own.at[r, pl.ds(mine, own_k), pl.ds(half, half)]

    def copy(name, r):
        if name == "b1":
            return remote(name, r, first(r), rp.at[r], pair)
        if name == "b3":
            return remote(name, r, second(r), rc.at[r], cross)
        if name == "a1":
            return remote(name, r, a.at[r], own.at[r, pl.ds(mine, own_k)], pair)
        if name == "a3":
            return remote(name, r, a.at[r], far.at[0, r, pl.ds(mine, own_k)], cross)
        if name == "r3":
            return remote(name, r, rp.at[r], far.at[0, r, pl.ds(other, own_k), pl.ds(0, half)], cross)
        if name == "r1":
            return remote(name, r, rc.at[r], far.at[0, r, pl.ds(other, own_k), pl.ds(half, half)], pair)
        if name == "z":
            return remote(name, r, far.at[0, r], far.at[1, r], z_to)
        if name == "do":
            return remote(name, r, own.at[r], po.at[r], twin)
        if name == "ds":
            return remote(name, r, far.at[side, r], ps.at[r], twin)
        here = whole.at[r, pl.ds(y * pair_k, pair_k)]
        if name == "yp":
            return remote(name, r, here, here, y_up)
        if name == "ym":
            return remote(name, r, here, here, y_down)
        if name == "qp":
            got = whole.at[r, pl.ds(down * pair_k, pair_k), pl.ds(0, half)]
            return remote(name, r, got, got, y_up)
        got = whole.at[r, pl.ds(up * pair_k, pair_k), pl.ds(half, half)]
        return remote(name, r, got, got, y_down)

    def load(r):
        return pltpu.make_async_copy(
            green.at[:, 0, :, pl.ds(r * ROWS, ROWS)], stage.at[:, :, pl.ds(r * ROWS, ROWS)], load_sem.at[r])

    def convert(r):
        rows = pl.ds(r * ROWS, ROWS)
        for j in range(own_k):
            a[r, j] = stage[j, 1 - part, rows].astype(BF)
            own[r, mine + j] = stage[j, part, rows].astype(BF)

    pl.loop(0, chunks)(lambda r: load(r).start())
    cload = pltpu.make_async_copy(coupling, cmat, cload_sem)
    cload.start()
    barrier = pltpu.get_barrier_semaphore()
    for device in (pair, cross, z_to, z_from, twin, y_up, y_down):
        pl.semaphore_signal(barrier, inc=1, device_id=device, device_id_type=MESH)

    @pl.loop(0, chunks)
    def _(r):
        load(r).wait()
        convert(r)

    pl.semaphore_wait(barrier, 7)

    def mix(r):
        for i in range(pair_k):
            total = weight[i, 0] * po[r, i].astype(F32)
            total += weight[i, 1] * ps[r, i].astype(F32)
            total += weight[i, 2] * far[0, r, i].astype(F32)
            total += weight[i, 3] * far[1, r, i].astype(F32)
            whole[r, y * pair_k + i] = total.astype(BF)

    def classes(b):
        @pl.loop(0, every_k)
        def _(s):
            for u in range(SUB):
                block[s, u * ROWS:(u + 1) * ROWS] = whole[b * SUB + u, s]

        tiles = height // 16

        @pl.loop(0, pair_k * tiles)
        def _(i):
            k, tile = i // tiles, i % tiles
            rows = pl.ds(pl.multiple_of(tile * 16, 16), 16)
            total = jnp.zeros((16, n), F32)
            for j in range(every_k):
                total += block[perm[k, j], rows].astype(F32)
                prefix[j + 1] = total
            low = prefix[ends[k, 0]]
            to = pl.ds(pl.multiple_of(i * 16, 16), 16)
            for q in range(nq):
                high = prefix[ends[k, q + 1]]
                bins[q, to] = (high - low).astype(BF)
                low = high

        @pl.loop(0, nq)
        def _(q):
            product = lax.dot_general(
                bins[q], cmat[q], (((1,), (1,)), ((), ())), preferred_element_type=F32).astype(BF)
            at = pl.ds(pl.multiple_of(q * height, height), height)
            for k in range(pair_k):
                right[k, at] = product[k * height:(k + 1) * height]

    def osend(j):
        return pltpu.make_async_remote_copy(
            src_ref=obf.at[j], dst_ref=orecv.at[j], send_sem=osend_sem.at[j], recv_sem=orecv_sem.at[j],
            device_id=pair, device_id_type=MESH)

    total_of = stage

    def close(b):
        @pl.loop(0, pair_k)
        def _(i):
            k = (other + i) % pair_k
            term = jnp.dot(cst[b], right[k], preferred_element_type=F32)

            @pl.when(b == 0)
            def _():
                total_of[k // 2, k % 2] = term

            @pl.when(b > 0)
            def _():
                total_of[k // 2, k % 2] += term

            @pl.when((b == blocks - 1) & (i < own_k))
            def _():
                obf[i] = (total_of[k // 2, k % 2] / every_k).astype(BF)

            @pl.when((b == blocks - 1) & (i >= 1) & (i < own_k + 1))
            def _():
                osend(i - 1).start()

    def when(ok, names, what):
        pl.when(ok)(lambda: what())

    def within(r):
        return (r >= 0) & (r < chunks)

    @pl.loop(0, chunks + 6)
    def _(t):
        @pl.when(within(t))
        def _():
            for name in ("b1", "b3", "a1", "a3"):
                copy(name, t).start()
            copy("b1", t).wait_recv()
            copy("r3", t).start()
            copy("b3", t).wait_recv()
            copy("r1", t).start()

        @pl.when(t == 0)
        def _():
            cload.wait()
            prefix[0] = jnp.zeros((16, n), F32)
            right[:, nq * height:] = jnp.zeros((pair_k, right.shape[1] - nq * height, n), BF)
            lane = lax.broadcasted_iota(jnp.int32, (n, 128), 1) < height

            @pl.loop(0, (nq + 1) // 2)
            def _(h):
                for d in range(n // 128):
                    lhs = cmat[2 * h, :, d * 128:(d + 1) * 128].astype(F32)
                    rhs = cmat[jnp.minimum(2 * h + 1, nq - 1), :, d * 128:(d + 1) * 128].astype(F32)
                    rhs = jnp.where(2 * h + 1 < nq, rhs, jnp.zeros_like(rhs))
                    to = pl.ds(pl.multiple_of(h * 128, 128), 128)
                    cst[2 * d, :, to] = jnp.where(lane, lhs, pltpu.roll(rhs, height, 1)).astype(BF)
                    cst[2 * d + 1, :, to] = jnp.where(lane, pltpu.roll(lhs, height, 1), rhs).astype(BF)

        @pl.when(within(t - 3))
        def _():
            r = t - 3
            copy("do", r).wait_recv()
            copy("ds", r).wait_recv()
            mix(r)

        @pl.when(within(t - 1))
        def _():
            r = t - 1
            copy("a3", r).wait_recv()
            copy("r3", r).wait_recv()
            copy("r1", r).wait_recv()
            copy("z", r).start()
            copy("a1", r).wait_recv()
            copy("do", r).start()

        @pl.when(within(t - 2))
        def _():
            r = t - 2
            copy("z", r).wait_recv()
            copy("ds", r).start()

        @pl.when(within(t - 3))
        def _():
            copy("yp", t - 3).start()
            copy("ym", t - 3).start()

        @pl.when(within(t - 4))
        def _():
            r = t - 4
            copy("yp", r).wait_recv()
            copy("qp", r).start()
            copy("ym", r).wait_recv()
            copy("qm", r).start()

        @pl.when(within(t - 5))
        def _():
            r = t - 5
            copy("qp", r).wait_recv()
            copy("qm", r).wait_recv()

            @pl.when(r % SUB == SUB - 1)
            def _():
                classes(r // SUB)

        @pl.when(within(t - 6) & ((t - 6) % SUB == SUB - 1))
        def _():
            close((t - 6) // SUB)

    for name, ref in (("b1", rp), ("b3", rc), ("a1", a), ("a3", a), ("r1", rc), ("r3", rp), ("z", far.at[0]),
                      ("do", own), ("ds", ps), ("yp", own), ("ym", own), ("qp", a), ("qm", a)):
        pltpu.make_async_copy(ref, ref, send_sem.at[kinds[name]]).wait()

    def store(j, p, k):
        return pltpu.make_async_copy(total_of.at[k // 2, k % 2], out.at[j, 0, p], store_sem.at[j, p])

    for j in range(own_k):
        k = mine + j
        total_of[k // 2, k % 2] = total_of[k // 2, k % 2] / every_k
        store(j, part, k).start()
    for j in range(own_k):
        k = other + j
        osend(j).wait_recv()
        total_of[k // 2, k % 2] = orecv[j].astype(F32)
        store(j, 1 - part, k).start()
    for j in range(own_k):
        osend(j).wait_send()
        store(j, part, mine + j).wait()
        store(j, 1 - part, other + j).wait()


def body(green_blocks, transfer_index, photon_shift, photon_occupancy, coupling):
    own_k, n = green_blocks.shape[0], green_blocks.shape[3]
    momenta, nq = transfer_index.shape[1], coupling.shape[0]
    pair_k = 2 * own_k
    chunks, height = n // ROWS, ROWS * SUB
    deep = (nq + 1) // 2 * 2 * height
    mom, en = lax.axis_index("mom"), lax.axis_index("en")
    count = lax.axis_size("en")
    xl = mom // NY
    xh, core = (en // 2) % 2, en % 2

    packed = jnp.concatenate([transfer_index, photon_shift[:, None]], axis=1)
    others = lax.ppermute(packed, "mom", [(i, (i + NY) % (NX * NY)) for i in range(NX * NY)])
    both = jnp.where(xl == 0, jnp.stack([packed, others]), jnp.stack([others, packed]))
    both = both.reshape(pair_k, momenta + 1)
    shift = both[:, momenta]
    table = both[:, :momenta].reshape(pair_k, NX, NY, own_k).transpose(0, 2, 1, 3).reshape(pair_k, momenta)
    slot = jnp.arange(momenta, dtype=jnp.int32)
    key = table * 64 + slot
    rank = jnp.sum((key[:, None, :] < key[:, :, None]).astype(jnp.int32), axis=2)
    perm = jnp.sum(jnp.where(rank[:, :, None] == slot, slot[None, :, None], 0), axis=1)
    ends = jnp.sum((table[:, None, :] < jnp.arange(nq + 1, dtype=jnp.int32)[None, :, None]).astype(jnp.int32), axis=2)
    occupy = photon_occupancy[0]
    near = shift == 1
    zero = jnp.zeros_like(occupy)
    below1 = jnp.where(near & (en >= 1), occupy, zero)
    above1 = jnp.where(near & (en + 1 < count), occupy + 1.0, zero)
    below2 = jnp.where(~near & (en >= 2), occupy, zero)
    above2 = jnp.where(~near & (en + 2 < count), occupy + 1.0, zero)
    weight = jnp.stack([
        jnp.where(core == 0, above1, below1), jnp.where(core == 0, below1, above1),
        jnp.where(xh == 0, above2, below2), jnp.where(xh == 0, below2, above2)], axis=1)

    smem = pl.BlockSpec(memory_space=pltpu.SMEM)
    hbm = pl.BlockSpec(memory_space=pl.ANY)
    dma = pltpu.SemaphoreType.DMA
    return pl.pallas_call(
        functools.partial(kernel, n, nq, own_k),
        out_shape=jax.ShapeDtypeStruct(green_blocks.shape, F32),
        in_specs=[smem, smem, smem, hbm, hbm],
        out_specs=hbm,
        scratch_shapes=[
            pltpu.VMEM((own_k, 2, n, n), F32),
            pltpu.VMEM((chunks, own_k, ROWS, n), BF),
            pltpu.VMEM((chunks, pair_k, ROWS, n), BF),
            pltpu.VMEM((2, chunks, pair_k, ROWS, n), BF),
            pltpu.VMEM((chunks, own_k, ROWS // 2, n), BF),
            pltpu.VMEM((chunks, own_k, ROWS // 2, n), BF),
            pltpu.VMEM((chunks, pair_k, ROWS, n), BF),
            pltpu.VMEM((chunks, pair_k, ROWS, n), BF),
            pltpu.VMEM((chunks, momenta, ROWS, n), BF),
            pltpu.VMEM((nq, n, n), BF),
            pltpu.VMEM((n // height, n, deep), BF),
            pltpu.VMEM((momenta, height, n), BF),
            pltpu.VMEM((momenta + 1, 16, n), F32),
            pltpu.VMEM((nq, pair_k * height, n), BF),
            pltpu.VMEM((pair_k, deep, n), BF),
            pltpu.VMEM((own_k, n, n), BF),
            pltpu.VMEM((own_k, n, n), BF),
            dma((chunks,)), dma(()), dma((len(RELAYED),)), dma((len(RELAYED), chunks)),
            dma((own_k,)), dma((own_k,)), dma((own_k, 2)),
        ],
        compiler_params=pltpu.CompilerParams(
            collective_id=0, has_side_effects=True, vmem_limit_bytes=67_043_328),
        name="scba",
    )(perm, ends, weight, green_blocks, coupling)


def solution(mesh):
    placed = (P("mom", "en", None, None, None), P("mom", None), P("mom"), P(), P())
    return jax.shard_map(
        body,
        mesh=mesh,
        in_specs=placed,
        out_specs=P("mom", "en", None, None, None),
        check_vma=False,
    )
```

```python
import functools

import jax
import jax.numpy as jnp
from jax import lax
from jax.experimental import pallas as pl
from jax.experimental.pallas import tpu as pltpu
from jax.sharding import PartitionSpec as P

MESH = pl.DeviceIdType.MESH
BF = jnp.bfloat16
F32 = jnp.float32

NX, NY, NZ = 2, 4, 4
ROWS = 32
SUB = 2
KSTEP = 3
QSTEP = 3
RELAYED = ("b1", "b3", "a1", "a3", "r1", "r3", "z", "do", "ds", "y1", "yx", "yf", "t0", "t1", "t2", "t3")


def kernel(n, nq, own_k, count, packed, occupancy, green, coupling, out,
           stage, a, own, far, rp, rc, po, ps, whole, cmat, cst, block, prefix, bins, right, tables, order,
           perm, ends, shifts,
           load_sem, cload_sem, send_sem, recv_sem, osend_sem, orecv_sem, table_send, table_recv, table_sem):
    chunks = n // ROWS
    half = ROWS // 2
    height = ROWS * SUB
    blocks = chunks // SUB
    pair_k = 2 * own_k
    every_k = NY * pair_k
    mom, en = lax.axis_index("mom"), lax.axis_index("en")
    xl, y = mom // NY, mom % NY
    z, xh, core = en // 4, (en // 2) % 2, en % 2
    part = xl
    mine, other = xl * own_k, (1 - xl) * own_k
    near, across = y + 1 - 2 * (y % 2), NY - 1 - y
    hub = core == y // 2
    helper = core != y // 2

    def place(axl, ay, az, axh, acore):
        return (axl * NY + ay, (az * 2 + axh) * 2 + acore)

    pair = place(1 - xl, y, z, xh, core)
    cross = place(1 - xl, y, z, 1 - xh, core)
    z_to = place(xl, y, (z + 1 + 2 * xh) % NZ, xh, core)
    z_from = place(xl, y, (z + 3 + 2 * xh) % NZ, xh, core)
    twin = place(xl, y, z, xh, 1 - core)
    y_near = place(xl, near, z, xh, core)
    y_across = place(xl, across, z, xh, core)
    corner = place(1 - xl, across, z, xh, core)
    o_across = place(xl, across, z, xh, 1 - core)
    o_corner = place(1 - xl, across, z, xh, 1 - core)
    side = (core + xh) % 2

    kinds = {name: i for i, name in enumerate(RELAYED)}

    def remote(name, r, src, dst, device):
        i = kinds[name]
        return pltpu.make_async_remote_copy(
            src_ref=src, dst_ref=dst, send_sem=send_sem.at[i], recv_sem=recv_sem.at[i, r],
            device_id=device, device_id_type=MESH)

    def first(r):
        return own.at[r, pl.ds(mine, own_k), pl.ds(0, half)]

    def second(r):
        return own.at[r, pl.ds(mine, own_k), pl.ds(half, half)]

    def copy(name, r):
        if name == "b1":
            return remote(name, r, first(r), rp.at[r], pair)
        if name == "b3":
            return remote(name, r, second(r), rc.at[r], cross)
        if name == "a1":
            return remote(name, r, a.at[r], own.at[r, pl.ds(mine, own_k)], pair)
        if name == "a3":
            return remote(name, r, a.at[r], far.at[0, r, pl.ds(mine, own_k)], cross)
        if name == "r3":
            return remote(name, r, rp.at[r], far.at[0, r, pl.ds(other, own_k), pl.ds(0, half)], cross)
        if name == "r1":
            return remote(name, r, rc.at[r], far.at[0, r, pl.ds(other, own_k), pl.ds(half, half)], pair)
        if name == "z":
            return remote(name, r, far.at[0, r], far.at[1, r], z_to)
        if name == "do":
            return remote(name, r, own.at[r], po.at[r], twin)
        if name == "ds":
            return remote(name, r, far.at[side, r], ps.at[r], twin)

        def group(g):
            return whole.at[r, pl.ds(g * pair_k, pair_k)]

        if name == "y1":
            return remote(name, r, group(y), group(y), y_near)
        if name == "yx":
            return remote(name, r, group(NY), group(y), y_across)
        if name == "yf":
            return remote(name, r, group(across), group(across), y_near)
        g = {"t0": y, "t1": near, "t2": across, "t3": NY - 1 - near}[name]
        return remote(name, r, group(g), group(g), twin)

    def load(r):
        return pltpu.make_async_copy(
            green.at[:, 0, :, pl.ds(r * ROWS, ROWS)], stage.at[:, :, pl.ds(r * ROWS, ROWS)], load_sem.at[r])

    def convert(r):
        rows = pl.ds(r * ROWS, ROWS)
        for j in range(own_k):
            a[r, j] = stage[j, 1 - part, rows].astype(BF)
            own[r, mine + j] = stage[j, part, rows].astype(BF)

    pl.loop(0, chunks)(lambda r: load(r).start())
    cload = pltpu.make_async_copy(coupling, cmat, cload_sem)
    cload.start()
    barrier = pltpu.get_barrier_semaphore()
    everyone = (pair, cross, z_to, z_from, twin, y_near, y_across, corner, o_across, o_corner)
    for device in everyone:
        pl.semaphore_signal(barrier, inc=1, device_id=device, device_id_type=MESH)

    @pl.loop(0, 2)
    def _(r):
        load(r).wait()
        convert(r)

    pl.semaphore_wait(barrier, len(everyone))

    def x_start(r):
        for name in ("b1", "b3", "a1", "a3"):
            copy(name, r).start()

    x_start(0)

    def table_copy(i, device, where):
        return pltpu.make_async_remote_copy(
            src_ref=packed, dst_ref=tables.at[where], send_sem=table_send.at[i], recv_sem=table_recv.at[i],
            device_id=device, device_id_type=MESH)

    sent_tables = [table_copy(0, pair, xl), table_copy(1, y_across, 2 + xl), table_copy(2, corner, 2 + xl)]
    for sent in sent_tables:
        sent.start()
    tables[xl] = packed[...]

    @pl.loop(2, chunks)
    def _(r):
        load(r).wait()
        convert(r)

    def sort_tables():
        for sent in sent_tables:
            sent.wait()
        lane = lax.broadcasted_iota(jnp.int32, (8, 128), 1)
        real = lane < every_k
        first_of = jnp.where(hub, 0, 2)
        slots = [c % (NY * own_k) // own_k * pair_k + c // (NY * own_k) * own_k + c % own_k for c in range(every_k)]
        slot = jnp.zeros((8, 128), jnp.int32)
        for c in range(every_k):
            slot = jnp.where(lane == c, slots[c], slot)
        for g in range(2):
            table = tables[first_of + g]
            key = table * 64 + slot
            rank = jnp.zeros((8, 128), jnp.int32)
            bound = jnp.zeros((8, 128), jnp.int32)
            for c in range(every_k):
                rank += jnp.where(key[:, c:c + 1] < key, 1, 0)
                bound += jnp.where(table[:, c:c + 1] < lane, 1, 0)
            place_of = jnp.zeros((8, 128), jnp.int32)
            for c in range(every_k):
                place_of += jnp.where((rank[:, c:c + 1] == lane) & real, slots[c], 0)
            order[g] = place_of
            order[2 + g] = bound
        copies = [
            pltpu.make_async_copy(order.at[pl.ds(0, 2)], perm, table_sem.at[0]),
            pltpu.make_async_copy(order.at[pl.ds(2, 2)], ends, table_sem.at[1]),
            pltpu.make_async_copy(tables.at[pl.ds(0, 2)], shifts, table_sem.at[2])]
        for c in copies:
            c.start()
        for c in copies:
            c.wait()

    low_occupancy = occupancy[0]
    high_occupancy = low_occupancy + 1.0

    def weights(i):
        shift = shifts[i // own_k, i % own_k, every_k]
        below1 = jnp.where((shift == 1) & (en >= 1), low_occupancy, 0.0)
        above1 = jnp.where((shift == 1) & (en + 1 < count), high_occupancy, 0.0)
        below2 = jnp.where((shift != 1) & (en >= 2), low_occupancy, 0.0)
        above2 = jnp.where((shift != 1) & (en + 2 < count), high_occupancy, 0.0)
        return (jnp.where(core == 0, above1, below1), jnp.where(core == 0, below1, above1),
                jnp.where(xh == 0, above2, below2), jnp.where(xh == 0, below2, above2))

    def mix(r):
        to = jnp.where(hub, y, NY) * pair_k
        for i in range(pair_k):
            w = weights(i)
            total = w[0] * po[r, i].astype(F32)
            total += w[1] * ps[r, i].astype(F32)
            total += w[2] * far[0, r, i].astype(F32)
            total += w[3] * far[1, r, i].astype(F32)
            whole[r, to + i] = total.astype(BF)

    total_of = stage
    tiles = height // 16

    def term(b, k):
        product = jnp.dot(cst[b], right[k], preferred_element_type=F32)
        total_of[k // 2, k % 2] = jnp.where(b == 0, product, total_of[k // 2, k % 2] + product)

    def bin_tile(k, tile):
        rows = pl.ds(tile * 16, 16)
        total = jnp.zeros((16, n), F32)
        for j in range(every_k):
            total += block[perm[k // own_k, k % own_k, j], rows].astype(F32)
            prefix[tile, j + 1] = total
        low = prefix[tile, ends[k // own_k, k % own_k, 0]]
        to = pl.ds(pl.multiple_of((k * tiles + tile) * 16, 16), 16)
        for q in range(nq):
            high = prefix[tile, ends[k // own_k, k % own_k, q + 1]]
            bins[q, to] = (high - low).astype(BF)
            low = high

    def classes(b):
        @pl.loop(0, every_k)
        def _(s):
            for u in range(SUB):
                block[s, u * ROWS:(u + 1) * ROWS] = whole[b * SUB + u, s]

        @pl.loop(0, pair_k, step=KSTEP)
        def _(k0):
            for k in range(KSTEP):
                term(b - 1, k0 + k)
                for tile in range(tiles):
                    bin_tile(k0 + k, tile)

    def classes0():
        @pl.loop(0, every_k)
        def _(s):
            for u in range(SUB):
                block[s, u * ROWS:(u + 1) * ROWS] = whole[u, s]

        @pl.loop(0, pair_k)
        def _(k):
            for tile in range(tiles):
                bin_tile(k, tile)

    def rights():
        @pl.loop(0, nq, step=QSTEP)
        def _(q0):
            for d in range(QSTEP):
                q = q0 + d
                product = lax.dot_general(
                    bins[q], cmat[q], (((1,), (1,)), ((), ())), preferred_element_type=F32).astype(BF)
                at = pl.ds(pl.multiple_of(q * height, height), height)
                for k in range(pair_k):
                    right[k, at] = product[k * height:(k + 1) * height]

    def osend(k, device):
        return pltpu.make_async_remote_copy(
            src_ref=own.at[:, k], dst_ref=out.at[k % own_k, part], send_sem=osend_sem.at[k],
            recv_sem=orecv_sem.at[mine + k % own_k], device_id=device, device_id_type=MESH)

    def keep(k):
        return pltpu.make_async_copy(own.at[:, k], out.at[k % own_k, part], osend_sem.at[k])

    def send_out(k):
        far_side = (k // own_k) != xl

        @pl.when(hub & jnp.logical_not(far_side))
        def _():
            keep(k).start()

        @pl.when(hub & far_side)
        def _():
            osend(k, pair).start()

        @pl.when(helper & far_side)
        def _():
            osend(k, o_corner).start()

        @pl.when(helper & jnp.logical_not(far_side))
        def _():
            osend(k, o_across).start()

    def all_sent(name, ref):
        pltpu.make_async_copy(ref, ref, send_sem.at[kinds[name]]).wait()

    def finish():
        for name, ref in (("b1", rp), ("b3", rc), ("do", own)):
            all_sent(name, ref)

        @pl.loop(0, pair_k)
        def _(i):
            k = (other + i) % pair_k
            product = jnp.dot(cst[blocks - 1], right[k], preferred_element_type=F32)
            product = (total_of[k // 2, k % 2] + product) * (1.0 / every_k)
            own[:, k] = product.astype(BF).reshape(chunks, ROWS, n)

            @pl.when(i >= 1)
            def _():
                send_out((other + i - 1) % pair_k)

        send_out((other + pair_k - 1) % pair_k)

    def within(r):
        return (r >= 0) & (r < chunks)

    @pl.loop(0, chunks + 6)
    def _(t):
        @pl.when(within(t))
        def _():
            copy("b1", t).wait_recv()
            copy("r3", t).start()
            copy("b3", t).wait_recv()
            copy("r1", t).start()

        @pl.when(within(t + 1))
        def _():
            x_start(t + 1)

        @pl.when(t == 0)
        def _():
            cload.wait()
            prefix[:, 0] = jnp.zeros((tiles, 16, n), F32)
            right[:, nq * height:] = jnp.zeros((pair_k, right.shape[1] - nq * height, n), BF)
            lane = lax.broadcasted_iota(jnp.int32, (n, 128), 1) < height

            @pl.loop(0, (nq + 1) // 2)
            def _(h):
                for d in range(n // 128):
                    lhs = cmat[2 * h, :, d * 128:(d + 1) * 128].astype(F32)
                    rhs = cmat[jnp.minimum(2 * h + 1, nq - 1), :, d * 128:(d + 1) * 128].astype(F32)
                    rhs = jnp.where(2 * h + 1 < nq, rhs, jnp.zeros_like(rhs))
                    to = pl.ds(pl.multiple_of(h * 128, 128), 128)
                    cst[2 * d, :, to] = jnp.where(lane, lhs, pltpu.roll(rhs, height, 1)).astype(BF)
                    cst[2 * d + 1, :, to] = jnp.where(lane, pltpu.roll(lhs, height, 1), rhs).astype(BF)

        @pl.when(t == 1)
        def _():
            sort_tables()

        @pl.when(within(t - 1))
        def _():
            r = t - 1
            copy("a3", r).wait_recv()
            copy("r3", r).wait_recv()
            copy("r1", r).wait_recv()
            copy("z", r).start()
            copy("a1", r).wait_recv()
            copy("do", r).start()

        @pl.when(within(t - 2))
        def _():
            r = t - 2
            copy("z", r).wait_recv()
            copy("ds", r).start()

        @pl.when(within(t - 5))
        def _():
            r = t - 5

            @pl.when(helper)
            def _():
                for name in ("t0", "t2", "t1", "t3"):
                    copy(name, r).wait_recv()

            @pl.when(r == SUB - 1)
            def _():
                classes0()

            @pl.when((r % SUB == SUB - 1) & (r >= SUB))
            def _():
                classes(r // SUB)

        @pl.when(within(t - 6) & ((t - 6) % SUB == SUB - 1))
        def _():
            rights()

        @pl.when(within(t - 3) & hub)
        def _():
            r = t - 3
            copy("yx", r).wait_recv()
            copy("yf", r).start()
            copy("t2", r).start()

        @pl.when(within(t - 4) & hub)
        def _():
            r = t - 4
            copy("y1", r).wait_recv()
            copy("t1", r).start()
            copy("yf", r).wait_recv()
            copy("t3", r).start()

        @pl.when(within(t - 2))
        def _():
            r = t - 2
            copy("do", r).wait_recv()
            copy("ds", r).wait_recv()
            mix(r)

        @pl.when(within(t - 2) & hub)
        def _():
            copy("y1", t - 2).start()
            copy("t0", t - 2).start()

        @pl.when(within(t - 2) & helper)
        def _():
            copy("yx", t - 2).start()

    finish()

    for name, ref in (("a1", a), ("a3", a), ("r1", rc), ("r3", rp), ("z", far.at[0]), ("ds", ps)):
        all_sent(name, ref)

    @pl.when(hub)
    def _():
        for name in ("y1", "yf", "t0", "t1", "t2", "t3"):
            all_sent(name, ps)

    @pl.when(helper)
    def _():
        all_sent("yx", ps)

    for k in range(pair_k):
        mine_too = hub & ((k // own_k) == xl)

        @pl.when(mine_too)
        def _():
            keep(k).wait()

        @pl.when(jnp.logical_not(mine_too))
        def _():
            osend(k, pair).wait_send()
    for p in range(2):
        for j in range(own_k):
            @pl.when(helper | (p != xl))
            def _():
                pltpu.make_async_copy(out.at[j, p], out.at[j, p], orecv_sem.at[p * own_k + j]).wait()


def body(green_blocks, transfer_index, photon_shift, photon_occupancy, coupling):
    own_k, n = green_blocks.shape[0], green_blocks.shape[3]
    momenta, nq = transfer_index.shape[1], coupling.shape[0]
    pair_k = 2 * own_k
    chunks, height = n // ROWS, ROWS * SUB
    deep = (nq + 1) // 2 * 2 * height
    count = lax.axis_size("en")
    packed = jnp.concatenate([transfer_index, photon_shift[:, None]], axis=1)
    packed = jnp.pad(packed, ((0, 8 - own_k), (0, 128 - momenta - 1)))

    smem = pl.BlockSpec(memory_space=pltpu.SMEM)
    hbm = pl.BlockSpec(memory_space=pl.ANY)
    dma = pltpu.SemaphoreType.DMA
    parts = pl.pallas_call(
        functools.partial(kernel, n, nq, own_k, count),
        out_shape=jax.ShapeDtypeStruct((own_k, 2, chunks, ROWS, n), BF),
        in_specs=[pl.BlockSpec(memory_space=pltpu.VMEM), smem, hbm, hbm],
        out_specs=hbm,
        scratch_shapes=[
            pltpu.VMEM((own_k, 2, n, n), F32),
            pltpu.VMEM((chunks, own_k, ROWS, n), BF),
            pltpu.VMEM((chunks, pair_k, ROWS, n), BF),
            pltpu.VMEM((2, chunks, pair_k, ROWS, n), BF),
            pltpu.VMEM((chunks, own_k, ROWS // 2, n), BF),
            pltpu.VMEM((chunks, own_k, ROWS // 2, n), BF),
            pltpu.VMEM((chunks, pair_k, ROWS, n), BF),
            pltpu.VMEM((chunks, pair_k, ROWS, n), BF),
            pltpu.VMEM((chunks, momenta + pair_k, ROWS, n), BF),
            pltpu.VMEM((nq, n, n), BF),
            pltpu.VMEM((n // height, n, deep), BF),
            pltpu.VMEM((momenta, height, n), BF),
            pltpu.VMEM((height // 16, momenta + 1, 16, n), F32),
            pltpu.VMEM((nq, pair_k * height, n), BF),
            pltpu.VMEM((pair_k, deep, n), BF),
            pltpu.VMEM((4, 8, 128), jnp.int32),
            pltpu.VMEM((4, 8, 128), jnp.int32),
            pltpu.SMEM((2, 8, 128), jnp.int32),
            pltpu.SMEM((2, 8, 128), jnp.int32),
            pltpu.SMEM((2, 8, 128), jnp.int32),
            dma((chunks,)), dma(()), dma((len(RELAYED),)), dma((len(RELAYED), chunks)),
            dma((pair_k,)), dma((pair_k,)), dma((3,)), dma((3,)), dma((3,)),
        ],
        compiler_params=pltpu.CompilerParams(
            collective_id=0, has_side_effects=True, vmem_limit_bytes=67_043_328),
        name="scba",
    )(packed, photon_occupancy, green_blocks, coupling)
    return parts.reshape(green_blocks.shape).astype(F32)


def solution(mesh):
    placed = (P("mom", "en", None, None, None), P("mom", None), P("mom"), P(), P())
    return jax.shard_map(
        body,
        mesh=mesh,
        in_specs=placed,
        out_specs=P("mom", "en", None, None, None),
        check_vma=False,
    )
```

```python
import functools

import jax
import jax.numpy as jnp
from jax import lax
from jax.experimental import pallas as pl
from jax.experimental.pallas import tpu as pltpu
from jax.sharding import PartitionSpec as P

MESH = pl.DeviceIdType.MESH
BF = jnp.bfloat16
F32 = jnp.float32

NX, NY, NZ = 2, 4, 4
ROWS = 32
SUB = 2
KSTEP = 3
QSTEP = 3
RELAYED = ("b1", "b3", "a1", "a3", "r1", "r3", "z", "do", "ds", "y1", "yx", "yf", "t0", "t1", "t2", "t3")


def kernel(n, nq, own_k, count, packed, occupancy, green, coupling, out,
           stage, a, own, far, rp, rc, po, ps, whole, cmat, cst, block, prefix, bins, right, tables, order,
           perm, ends, shifts,
           load_sem, cload_sem, send_sem, recv_sem, osend_sem, orecv_sem, table_send, table_recv, table_sem):
    chunks = n // ROWS
    half = n // 2
    height = ROWS * SUB
    blocks = chunks // SUB
    pair_k = 2 * own_k
    every_k = NY * pair_k
    mom, en = lax.axis_index("mom"), lax.axis_index("en")
    xl, y = mom // NY, mom % NY
    z, xh, core = en // 4, (en // 2) % 2, en % 2
    part = xl
    mine, other = xl * own_k, (1 - xl) * own_k
    near, across = y + 1 - 2 * (y % 2), NY - 1 - y
    hub = core == y // 2
    helper = core != y // 2

    def place(axl, ay, az, axh, acore):
        return (axl * NY + ay, (az * 2 + axh) * 2 + acore)

    pair = place(1 - xl, y, z, xh, core)
    cross = place(1 - xl, y, z, 1 - xh, core)
    z_to = place(xl, y, (z + 1 + 2 * xh) % NZ, xh, core)
    z_from = place(xl, y, (z + 3 + 2 * xh) % NZ, xh, core)
    twin = place(xl, y, z, xh, 1 - core)
    y_near = place(xl, near, z, xh, core)
    y_across = place(xl, across, z, xh, core)
    corner = place(1 - xl, across, z, xh, core)
    o_across = place(xl, across, z, xh, 1 - core)
    o_corner = place(1 - xl, across, z, xh, 1 - core)
    side = (core + xh) % 2

    kinds = {name: i for i, name in enumerate(RELAYED)}

    def remote(name, r, src, dst, device):
        i = kinds[name]
        return pltpu.make_async_remote_copy(
            src_ref=src, dst_ref=dst, send_sem=send_sem.at[i], recv_sem=recv_sem.at[i, r],
            device_id=device, device_id_type=MESH)

    def first(r):
        return own.at[r, pl.ds(mine, own_k), :, pl.ds(0, half)]

    def second(r):
        return own.at[r, pl.ds(mine, own_k), :, pl.ds(half, half)]

    def copy(name, r):
        if name == "b1":
            return remote(name, r, first(r), rp.at[r], pair)
        if name == "b3":
            return remote(name, r, second(r), rc.at[r], cross)
        if name == "a1":
            return remote(name, r, a.at[r], own.at[r, pl.ds(mine, own_k)], pair)
        if name == "a3":
            return remote(name, r, a.at[r], far.at[0, r, pl.ds(mine, own_k)], cross)
        if name == "r3":
            return remote(name, r, rp.at[r], far.at[0, r, pl.ds(other, own_k), :, pl.ds(0, half)], cross)
        if name == "r1":
            return remote(name, r, rc.at[r], far.at[0, r, pl.ds(other, own_k), :, pl.ds(half, half)], pair)
        if name == "z":
            return remote(name, r, far.at[0, r], far.at[1, r], z_to)
        if name == "do":
            return remote(name, r, own.at[r], po.at[r], twin)
        if name == "ds":
            return remote(name, r, far.at[side, r], ps.at[r], twin)

        def group(g):
            return whole.at[r, pl.ds(g * pair_k, pair_k)]

        if name == "y1":
            return remote(name, r, group(y), group(y), y_near)
        if name == "yx":
            return remote(name, r, group(NY), group(y), y_across)
        if name == "yf":
            return remote(name, r, group(across), group(across), y_near)
        g = {"t0": y, "t1": near, "t2": across, "t3": NY - 1 - near}[name]
        return remote(name, r, group(g), group(g), twin)

    def load(r):
        return pltpu.make_async_copy(
            green.at[:, 0, :, pl.ds(r * ROWS, ROWS)], stage.at[:, :, pl.ds(r * ROWS, ROWS)], load_sem.at[r])

    def convert(r):
        rows = pl.ds(r * ROWS, ROWS)
        for j in range(own_k):
            a[r, j] = stage[j, 1 - part, rows].astype(BF)
            own[r, mine + j] = stage[j, part, rows].astype(BF)

    pl.loop(0, chunks)(lambda r: load(r).start())
    cload = pltpu.make_async_copy(coupling, cmat, cload_sem)
    cload.start()
    barrier = pltpu.get_barrier_semaphore()
    everyone = (pair, cross, z_to, z_from, twin, y_near, y_across, corner, o_across, o_corner)
    for device in everyone:
        pl.semaphore_signal(barrier, inc=1, device_id=device, device_id_type=MESH)

    @pl.loop(0, 2)
    def _(r):
        load(r).wait()
        convert(r)

    pl.semaphore_wait(barrier, len(everyone))

    def x_start(r):
        for name in ("b1", "b3", "a1", "a3"):
            copy(name, r).start()

    x_start(0)

    def table_copy(i, device, where):
        return pltpu.make_async_remote_copy(
            src_ref=packed, dst_ref=tables.at[where], send_sem=table_send.at[i], recv_sem=table_recv.at[i],
            device_id=device, device_id_type=MESH)

    sent_tables = [table_copy(0, pair, xl), table_copy(1, y_across, 2 + xl), table_copy(2, corner, 2 + xl)]
    for sent in sent_tables:
        sent.start()
    tables[xl] = packed[...]

    @pl.loop(2, chunks)
    def _(r):
        load(r).wait()
        convert(r)

    def sort_tables():
        for sent in sent_tables:
            sent.wait()
        lane = lax.broadcasted_iota(jnp.int32, (8, 128), 1)
        real = lane < every_k
        first_of = jnp.where(hub, 0, 2)
        slots = [c % (NY * own_k) // own_k * pair_k + c // (NY * own_k) * own_k + c % own_k for c in range(every_k)]
        slot = jnp.zeros((8, 128), jnp.int32)
        for c in range(every_k):
            slot = jnp.where(lane == c, slots[c], slot)
        for g in range(2):
            table = tables[first_of + g]
            key = table * 64 + slot
            rank = jnp.zeros((8, 128), jnp.int32)
            bound = jnp.zeros((8, 128), jnp.int32)
            for c in range(every_k):
                rank += jnp.where(key[:, c:c + 1] < key, 1, 0)
                bound += jnp.where(table[:, c:c + 1] < lane, 1, 0)
            place_of = jnp.zeros((8, 128), jnp.int32)
            for c in range(every_k):
                place_of += jnp.where((rank[:, c:c + 1] == lane) & real, slots[c], 0)
            order[g] = place_of
            order[2 + g] = bound
        copies = [
            pltpu.make_async_copy(order.at[pl.ds(0, 2)], perm, table_sem.at[0]),
            pltpu.make_async_copy(order.at[pl.ds(2, 2)], ends, table_sem.at[1]),
            pltpu.make_async_copy(tables.at[pl.ds(0, 2)], shifts, table_sem.at[2])]
        for c in copies:
            c.start()
        for c in copies:
            c.wait()

    low_occupancy = occupancy[0]
    high_occupancy = low_occupancy + 1.0

    def weights(i):
        shift = shifts[i // own_k, i % own_k, every_k]
        below1 = jnp.where((shift == 1) & (en >= 1), low_occupancy, 0.0)
        above1 = jnp.where((shift == 1) & (en + 1 < count), high_occupancy, 0.0)
        below2 = jnp.where((shift != 1) & (en >= 2), low_occupancy, 0.0)
        above2 = jnp.where((shift != 1) & (en + 2 < count), high_occupancy, 0.0)
        return (jnp.where(core == 0, above1, below1), jnp.where(core == 0, below1, above1),
                jnp.where(xh == 0, above2, below2), jnp.where(xh == 0, below2, above2))

    def mix(r):
        to = jnp.where(hub, y, NY) * pair_k
        for i in range(pair_k):
            w = weights(i)
            total = w[0] * po[r, i].astype(F32)
            total += w[1] * ps[r, i].astype(F32)
            total += w[2] * far[0, r, i].astype(F32)
            total += w[3] * far[1, r, i].astype(F32)
            whole[r, to + i] = total.astype(BF)

    total_of = stage
    tiles = height // 16

    def term(b, k):
        product = jnp.dot(cst[b], right[k], preferred_element_type=F32)
        total_of[k // 2, k % 2] = jnp.where(b == 0, product, total_of[k // 2, k % 2] + product)

    def bin_tile(k, tile):
        rows = pl.ds(tile * 16, 16)
        total = jnp.zeros((16, n), F32)
        for j in range(every_k):
            total += block[perm[k // own_k, k % own_k, j], rows].astype(F32)
            prefix[tile, j + 1] = total
        low = prefix[tile, ends[k // own_k, k % own_k, 0]]
        to = pl.ds(pl.multiple_of((k * tiles + tile) * 16, 16), 16)
        for q in range(nq):
            high = prefix[tile, ends[k // own_k, k % own_k, q + 1]]
            bins[q, to] = (high - low).astype(BF)
            low = high

    def take(b):
        @pl.loop(0, every_k)
        def _(s):
            for u in range(SUB):
                block[s, u * ROWS:(u + 1) * ROWS] = whole[b * SUB + u, s]

    def classes(b, k0):
        for k in range(k0, k0 + own_k):
            term(b - 1, k)
            for tile in range(tiles):
                bin_tile(k, tile)

    def classes0():
        @pl.loop(0, pair_k)
        def _(k):
            for tile in range(tiles):
                bin_tile(k, tile)

    def rights():
        @pl.loop(0, nq, step=QSTEP)
        def _(q0):
            for d in range(QSTEP):
                q = q0 + d
                product = lax.dot_general(
                    bins[q], cmat[q], (((1,), (1,)), ((), ())), preferred_element_type=F32).astype(BF)
                at = pl.ds(pl.multiple_of(q * height, height), height)
                for k in range(pair_k):
                    right[k, at] = product[k * height:(k + 1) * height]

    def osend(k, device):
        return pltpu.make_async_remote_copy(
            src_ref=own.at[:, k], dst_ref=out.at[k % own_k, part], send_sem=osend_sem.at[k],
            recv_sem=orecv_sem.at[mine + k % own_k], device_id=device, device_id_type=MESH)

    def keep(k):
        return pltpu.make_async_copy(own.at[:, k], out.at[k % own_k, part], osend_sem.at[k])

    def send_out(k):
        far_side = (k // own_k) != xl

        @pl.when(hub & jnp.logical_not(far_side))
        def _():
            keep(k).start()

        @pl.when(hub & far_side)
        def _():
            osend(k, pair).start()

        @pl.when(helper & far_side)
        def _():
            osend(k, o_corner).start()

        @pl.when(helper & jnp.logical_not(far_side))
        def _():
            osend(k, o_across).start()

    def all_sent(name, ref):
        pltpu.make_async_copy(ref, ref, send_sem.at[kinds[name]]).wait()

    def finish():
        for name, ref in (("b1", rp), ("b3", rc), ("do", own)):
            all_sent(name, ref)

        @pl.loop(0, pair_k)
        def _(i):
            k = (other + i) % pair_k
            product = jnp.dot(cst[blocks - 1], right[k], preferred_element_type=F32)
            product = (total_of[k // 2, k % 2] + product) * (1.0 / every_k)
            own[:, k] = product.astype(BF).reshape(chunks, ROWS, n)

            @pl.when(i >= 1)
            def _():
                send_out((other + i - 1) % pair_k)

        send_out((other + pair_k - 1) % pair_k)

    def within(r):
        return (r >= 0) & (r < chunks)

    @pl.loop(0, chunks + 8)
    def _(t):
        @pl.when(within(t - 4))
        def _():
            r = t - 4
            copy("do", r).wait_recv()
            copy("ds", r).wait_recv()
            mix(r)

        @pl.when(within(t - 4) & hub)
        def _():
            copy("y1", t - 4).start()
            copy("t0", t - 4).start()

        @pl.when(within(t - 4) & helper)
        def _():
            copy("yx", t - 4).start()

        @pl.when(within(t))
        def _():
            copy("b1", t).wait_recv()
            copy("r3", t).start()
            copy("b3", t).wait_recv()
            copy("r1", t).start()

        @pl.when(within(t + 1))
        def _():
            x_start(t + 1)

        @pl.when(t == 0)
        def _():
            cload.wait()
            prefix[:, 0] = jnp.zeros((tiles, 16, n), F32)
            right[:, nq * height:] = jnp.zeros((pair_k, right.shape[1] - nq * height, n), BF)
            lane = lax.broadcasted_iota(jnp.int32, (n, 128), 1) < height

            @pl.loop(0, (nq + 1) // 2)
            def _(h):
                for d in range(n // 128):
                    lhs = cmat[2 * h, :, d * 128:(d + 1) * 128].astype(F32)
                    rhs = cmat[jnp.minimum(2 * h + 1, nq - 1), :, d * 128:(d + 1) * 128].astype(F32)
                    rhs = jnp.where(2 * h + 1 < nq, rhs, jnp.zeros_like(rhs))
                    to = pl.ds(pl.multiple_of(h * 128, 128), 128)
                    cst[2 * d, :, to] = jnp.where(lane, lhs, pltpu.roll(rhs, height, 1)).astype(BF)
                    cst[2 * d + 1, :, to] = jnp.where(lane, pltpu.roll(lhs, height, 1), rhs).astype(BF)

        @pl.when(t == 1)
        def _():
            sort_tables()

        @pl.when(within(t - 1))
        def _():
            r = t - 1
            copy("a3", r).wait_recv()
            copy("r3", r).wait_recv()
            copy("r1", r).wait_recv()
            copy("z", r).start()
            copy("a1", r).wait_recv()
            copy("do", r).start()

        @pl.when(within(t - 3))
        def _():
            r = t - 3
            copy("z", r).wait_recv()
            copy("ds", r).start()

        @pl.when(within(t - 7))
        def _():
            r = t - 7

            @pl.when(helper)
            def _():
                for name in ("t0", "t2", "t1", "t3"):
                    copy(name, r).wait_recv()

            @pl.when(r % SUB == SUB - 1)
            def _():
                take(r // SUB)

            @pl.when(r == SUB - 1)
            def _():
                classes0()

            @pl.when((r % SUB == SUB - 1) & (r >= SUB))
            def _():
                classes(r // SUB, 0)
                classes(r // SUB, own_k)

        @pl.when(within(t - 8) & ((t - 8) % SUB == SUB - 1))
        def _():
            rights()

        @pl.when(within(t - 5) & hub)
        def _():
            r = t - 5
            copy("yx", r).wait_recv()
            copy("yf", r).start()
            copy("t2", r).start()

        @pl.when(within(t - 6) & hub)
        def _():
            r = t - 6
            copy("y1", r).wait_recv()
            copy("t1", r).start()
            copy("yf", r).wait_recv()
            copy("t3", r).start()

    finish()

    for name, ref in (("a1", a), ("a3", a), ("r1", rc), ("r3", rp), ("z", far.at[0]), ("ds", ps)):
        all_sent(name, ref)

    @pl.when(hub)
    def _():
        for name in ("y1", "yf", "t0", "t1", "t2", "t3"):
            all_sent(name, ps)

    @pl.when(helper)
    def _():
        all_sent("yx", ps)

    for k in range(pair_k):
        mine_too = hub & ((k // own_k) == xl)

        @pl.when(mine_too)
        def _():
            keep(k).wait()

        @pl.when(jnp.logical_not(mine_too))
        def _():
            osend(k, pair).wait_send()
    for p in range(2):
        for j in range(own_k):
            @pl.when(helper | (p != xl))
            def _():
                pltpu.make_async_copy(out.at[j, p], out.at[j, p], orecv_sem.at[p * own_k + j]).wait()


def body(green_blocks, transfer_index, photon_shift, photon_occupancy, coupling):
    own_k, n = green_blocks.shape[0], green_blocks.shape[3]
    momenta, nq = transfer_index.shape[1], coupling.shape[0]
    pair_k = 2 * own_k
    chunks, height = n // ROWS, ROWS * SUB
    deep = (nq + 1) // 2 * 2 * height
    count = lax.axis_size("en")
    packed = jnp.concatenate([transfer_index, photon_shift[:, None]], axis=1)
    packed = jnp.pad(packed, ((0, 8 - own_k), (0, 128 - momenta - 1)))

    smem = pl.BlockSpec(memory_space=pltpu.SMEM)
    hbm = pl.BlockSpec(memory_space=pl.ANY)
    dma = pltpu.SemaphoreType.DMA
    parts = pl.pallas_call(
        functools.partial(kernel, n, nq, own_k, count),
        out_shape=jax.ShapeDtypeStruct((own_k, 2, chunks, ROWS, n), BF),
        in_specs=[pl.BlockSpec(memory_space=pltpu.VMEM), smem, hbm, hbm],
        out_specs=hbm,
        scratch_shapes=[
            pltpu.VMEM((own_k, 2, n, n), F32),
            pltpu.VMEM((chunks, own_k, ROWS, n), BF),
            pltpu.VMEM((chunks, pair_k, ROWS, n), BF),
            pltpu.VMEM((2, chunks, pair_k, ROWS, n), BF),
            pltpu.VMEM((chunks, own_k, ROWS, n // 2), BF),
            pltpu.VMEM((chunks, own_k, ROWS, n // 2), BF),
            pltpu.VMEM((chunks, pair_k, ROWS, n), BF),
            pltpu.VMEM((chunks, pair_k, ROWS, n), BF),
            pltpu.VMEM((chunks, momenta + pair_k, ROWS, n), BF),
            pltpu.VMEM((nq, n, n), BF),
            pltpu.VMEM((n // height, n, deep), BF),
            pltpu.VMEM((momenta, height, n), BF),
            pltpu.VMEM((height // 16, momenta + 1, 16, n), F32),
            pltpu.VMEM((nq, pair_k * height, n), BF),
            pltpu.VMEM((pair_k, deep, n), BF),
            pltpu.VMEM((4, 8, 128), jnp.int32),
            pltpu.VMEM((4, 8, 128), jnp.int32),
            pltpu.SMEM((2, 8, 128), jnp.int32),
            pltpu.SMEM((2, 8, 128), jnp.int32),
            pltpu.SMEM((2, 8, 128), jnp.int32),
            dma((chunks,)), dma(()), dma((len(RELAYED),)), dma((len(RELAYED), chunks)),
            dma((pair_k,)), dma((pair_k,)), dma((3,)), dma((3,)), dma((3,)),
        ],
        compiler_params=pltpu.CompilerParams(
            collective_id=0, has_side_effects=True, vmem_limit_bytes=67_043_328),
        name="scba",
    )(packed, photon_occupancy, green_blocks, coupling)
    return parts.reshape(green_blocks.shape).astype(F32)


def solution(mesh):
    placed = (P("mom", "en", None, None, None), P("mom", None), P("mom"), P(), P())
    return jax.shard_map(
        body,
        mesh=mesh,
        in_specs=placed,
        out_specs=P("mom", "en", None, None, None),
        check_vma=False,
    )
```

```python
import functools

import jax
import jax.numpy as jnp
from jax import lax
from jax.experimental import pallas as pl
from jax.experimental.pallas import tpu as pltpu
from jax.sharding import PartitionSpec as P

MESH = pl.DeviceIdType.MESH
BF = jnp.bfloat16
F32 = jnp.float32

NX, NY, NZ = 2, 4, 4
ROWS = 32
SUB = 2
KSTEP = 3
QSTEP = 3
RELAYED = ("b1", "b3", "a1", "a3", "r1", "r3", "z", "do", "ds", "y1", "yx", "yf", "t0", "t1", "t2", "t3")


def kernel(n, nq, own_k, count, classes_in, shift_in, occupancy, green, coupling, out,
           stage, a, own, far, rp, rc, po, ps, whole, cmat, cst, block, prefix, bins, right, packed, tables, order,
           perm, ends, shifts,
           load_sem, cload_sem, send_sem, recv_sem, osend_sem, orecv_sem, table_send, table_recv, table_sem):
    chunks = n // ROWS
    half = n // 2
    height = ROWS * SUB
    blocks = chunks // SUB
    pair_k = 2 * own_k
    every_k = NY * pair_k
    mom, en = lax.axis_index("mom"), lax.axis_index("en")
    xl, y = mom // NY, mom % NY
    z, xh, core = en // 4, (en // 2) % 2, en % 2
    part = xl
    mine, other = xl * own_k, (1 - xl) * own_k
    near, across = y + 1 - 2 * (y % 2), NY - 1 - y
    hub = core == y // 2
    helper = core != y // 2

    def place(axl, ay, az, axh, acore):
        return (axl * NY + ay, (az * 2 + axh) * 2 + acore)

    pair = place(1 - xl, y, z, xh, core)
    cross = place(1 - xl, y, z, 1 - xh, core)
    z_to = place(xl, y, (z + 1 + 2 * xh) % NZ, xh, core)
    z_from = place(xl, y, (z + 3 + 2 * xh) % NZ, xh, core)
    twin = place(xl, y, z, xh, 1 - core)
    y_near = place(xl, near, z, xh, core)
    y_across = place(xl, across, z, xh, core)
    corner = place(1 - xl, across, z, xh, core)
    o_across = place(xl, across, z, xh, 1 - core)
    o_corner = place(1 - xl, across, z, xh, 1 - core)
    side = (core + xh) % 2

    kinds = {name: i for i, name in enumerate(RELAYED)}

    def remote(name, r, src, dst, device):
        i = kinds[name]
        return pltpu.make_async_remote_copy(
            src_ref=src, dst_ref=dst, send_sem=send_sem.at[i], recv_sem=recv_sem.at[i, r],
            device_id=device, device_id_type=MESH)

    def first(r):
        return own.at[r, pl.ds(mine, own_k), :, pl.ds(0, half)]

    def second(r):
        return own.at[r, pl.ds(mine, own_k), :, pl.ds(half, half)]

    def copy(name, r):
        if name == "b1":
            return remote(name, r, first(r), rp.at[r], pair)
        if name == "b3":
            return remote(name, r, second(r), rc.at[r], cross)
        if name == "a1":
            return remote(name, r, a.at[r], own.at[r, pl.ds(mine, own_k)], pair)
        if name == "a3":
            return remote(name, r, a.at[r], far.at[0, r, pl.ds(mine, own_k)], cross)
        if name == "r3":
            return remote(name, r, rp.at[r], far.at[0, r, pl.ds(other, own_k), :, pl.ds(0, half)], cross)
        if name == "r1":
            return remote(name, r, rc.at[r], far.at[0, r, pl.ds(other, own_k), :, pl.ds(half, half)], pair)
        if name == "z":
            return remote(name, r, far.at[0, r], far.at[1, r], z_to)
        if name == "do":
            return remote(name, r, own.at[r], po.at[r], twin)
        if name == "ds":
            return remote(name, r, far.at[side, r], ps.at[r], twin)

        def group(g):
            return whole.at[r, pl.ds(g * pair_k, pair_k)]

        if name == "y1":
            return remote(name, r, group(y), group(y), y_near)
        if name == "yx":
            return remote(name, r, group(NY), group(y), y_across)
        if name == "yf":
            return remote(name, r, group(across), group(across), y_near)
        g = {"t0": y, "t1": near, "t2": across, "t3": NY - 1 - near}[name]
        return remote(name, r, group(g), group(g), twin)

    def load(r):
        return pltpu.make_async_copy(
            green.at[:, 0, :, pl.ds(r * ROWS, ROWS)], stage.at[:, :, pl.ds(r * ROWS, ROWS)], load_sem.at[r])

    def convert(r):
        rows = pl.ds(r * ROWS, ROWS)
        for j in range(own_k):
            a[r, j] = stage[j, 1 - part, rows].astype(BF)
            own[r, mine + j] = stage[j, part, rows].astype(BF)

    pl.loop(0, chunks)(lambda r: load(r).start())
    cload = pltpu.make_async_copy(coupling, cmat, cload_sem)
    cload.start()
    row8 = lax.broadcasted_iota(jnp.int32, (8, 128), 0)
    lane8 = lax.broadcasted_iota(jnp.int32, (8, 128), 1)
    shifted = jnp.zeros((8, 128), jnp.int32)
    for j in range(own_k):
        shifted = jnp.where((row8 == j) & (lane8 == every_k), shift_in[j], shifted)
    packed[...] = shifted
    packed[0:own_k, 0:every_k] = classes_in[...]
    barrier = pltpu.get_barrier_semaphore()
    everyone = (pair, cross, z_to, z_from, twin, y_near, y_across, corner, o_across, o_corner)
    for device in everyone:
        pl.semaphore_signal(barrier, inc=1, device_id=device, device_id_type=MESH)

    @pl.loop(0, 2)
    def _(r):
        load(r).wait()
        convert(r)

    pl.semaphore_wait(barrier, len(everyone))

    def x_start(r):
        for name in ("b1", "b3", "a1", "a3"):
            copy(name, r).start()

    x_start(0)
    x_start(1)

    def table_copy(i, device, where):
        return pltpu.make_async_remote_copy(
            src_ref=packed, dst_ref=tables.at[where], send_sem=table_send.at[i], recv_sem=table_recv.at[i],
            device_id=device, device_id_type=MESH)

    sent_tables = [table_copy(0, pair, xl), table_copy(1, y_across, 2 + xl), table_copy(2, corner, 2 + xl)]
    for sent in sent_tables:
        sent.start()
    tables[xl] = packed[...]

    @pl.loop(2, chunks)
    def _(r):
        load(r).wait()
        convert(r)

    def sort_tables():
        for sent in sent_tables:
            sent.wait()
        lane = lax.broadcasted_iota(jnp.int32, (8, 128), 1)
        real = lane < every_k
        first_of = jnp.where(hub, 0, 2)
        slots = [c % (NY * own_k) // own_k * pair_k + c // (NY * own_k) * own_k + c % own_k for c in range(every_k)]
        slot = jnp.zeros((8, 128), jnp.int32)
        for c in range(every_k):
            slot = jnp.where(lane == c, slots[c], slot)
        for g in range(2):
            table = tables[first_of + g]
            key = table * 64 + slot
            rank = jnp.zeros((8, 128), jnp.int32)
            bound = jnp.zeros((8, 128), jnp.int32)
            for c in range(every_k):
                rank += jnp.where(key[:, c:c + 1] < key, 1, 0)
                bound += jnp.where(table[:, c:c + 1] < lane, 1, 0)
            place_of = jnp.zeros((8, 128), jnp.int32)
            for c in range(every_k):
                place_of += jnp.where((rank[:, c:c + 1] == lane) & real, slots[c], 0)
            order[g] = place_of
            order[2 + g] = bound
        copies = [
            pltpu.make_async_copy(order.at[pl.ds(0, 2)], perm, table_sem.at[0]),
            pltpu.make_async_copy(order.at[pl.ds(2, 2)], ends, table_sem.at[1]),
            pltpu.make_async_copy(tables.at[pl.ds(0, 2)], shifts, table_sem.at[2])]
        for c in copies:
            c.start()
        for c in copies:
            c.wait()

    low_occupancy = occupancy[0]
    high_occupancy = low_occupancy + 1.0

    def weights(i):
        shift = shifts[i // own_k, i % own_k, every_k]
        below1 = jnp.where((shift == 1) & (en >= 1), low_occupancy, 0.0)
        above1 = jnp.where((shift == 1) & (en + 1 < count), high_occupancy, 0.0)
        below2 = jnp.where((shift != 1) & (en >= 2), low_occupancy, 0.0)
        above2 = jnp.where((shift != 1) & (en + 2 < count), high_occupancy, 0.0)
        return (jnp.where(core == 0, above1, below1), jnp.where(core == 0, below1, above1),
                jnp.where(xh == 0, above2, below2), jnp.where(xh == 0, below2, above2))

    def mix(r):
        to = jnp.where(hub, y, NY) * pair_k
        for i in range(pair_k):
            w = weights(i)
            total = w[0] * po[r, i].astype(F32)
            total += w[1] * ps[r, i].astype(F32)
            total += w[2] * far[0, r, i].astype(F32)
            total += w[3] * far[1, r, i].astype(F32)
            whole[r, to + i] = total.astype(BF)

    total_of = stage
    tiles = height // 16

    def term(b, k):
        product = jnp.dot(cst[b], right[k], preferred_element_type=F32)
        total_of[k // 2, k % 2] = jnp.where(b == 0, product, total_of[k // 2, k % 2] + product)

    def bin_tile(k, tile):
        rows = pl.ds(tile * 16, 16)
        total = jnp.zeros((16, n), F32)
        for j in range(every_k):
            total += block[perm[k // own_k, k % own_k, j], rows].astype(F32)
            prefix[tile, j + 1] = total
        low = prefix[tile, ends[k // own_k, k % own_k, 0]]
        to = pl.ds(pl.multiple_of((k * tiles + tile) * 16, 16), 16)
        for q in range(nq):
            high = prefix[tile, ends[k // own_k, k % own_k, q + 1]]
            bins[q, to] = (high - low).astype(BF)
            low = high

    def take(b):
        @pl.loop(0, every_k)
        def _(s):
            for u in range(SUB):
                block[s, u * ROWS:(u + 1) * ROWS] = whole[b * SUB + u, s]

    def classes(b, k0):
        for k in range(k0, k0 + own_k):
            term(b - 1, k)
            for tile in range(tiles):
                bin_tile(k, tile)

    def classes0():
        @pl.loop(0, pair_k)
        def _(k):
            for tile in range(tiles):
                bin_tile(k, tile)

    def rights():
        @pl.loop(0, nq, step=QSTEP)
        def _(q0):
            for d in range(QSTEP):
                q = q0 + d
                product = lax.dot_general(
                    bins[q], cmat[q], (((1,), (1,)), ((), ())), preferred_element_type=F32).astype(BF)
                at = pl.ds(pl.multiple_of(q * height, height), height)
                for k in range(pair_k):
                    right[k, at] = product[k * height:(k + 1) * height]

    def osend(k, device):
        return pltpu.make_async_remote_copy(
            src_ref=own.at[:, k], dst_ref=out.at[k % own_k, part], send_sem=osend_sem.at[k],
            recv_sem=orecv_sem.at[mine + k % own_k], device_id=device, device_id_type=MESH)

    def keep(k):
        return pltpu.make_async_copy(own.at[:, k], out.at[k % own_k, part], osend_sem.at[k])

    def send_out(k):
        far_side = (k // own_k) != xl

        @pl.when(hub & jnp.logical_not(far_side))
        def _():
            keep(k).start()

        @pl.when(hub & far_side)
        def _():
            osend(k, pair).start()

        @pl.when(helper & far_side)
        def _():
            osend(k, o_corner).start()

        @pl.when(helper & jnp.logical_not(far_side))
        def _():
            osend(k, o_across).start()

    def all_sent(name, ref):
        pltpu.make_async_copy(ref, ref, send_sem.at[kinds[name]]).wait()

    def finish():
        for name, ref in (("b1", rp), ("b3", rc), ("do", own)):
            all_sent(name, ref)

        @pl.loop(0, pair_k)
        def _(i):
            k = (other + i) % pair_k
            product = jnp.dot(cst[blocks - 1], right[k], preferred_element_type=F32)
            product = (total_of[k // 2, k % 2] + product) * (1.0 / every_k)
            own[:, k] = product.astype(BF).reshape(chunks, ROWS, n)

            @pl.when(i >= 1)
            def _():
                send_out((other + i - 1) % pair_k)

        send_out((other + pair_k - 1) % pair_k)

    def within(r):
        return (r >= 0) & (r < chunks)

    @pl.loop(0, chunks + 8)
    def _(t):
        @pl.when(within(t - 4))
        def _():
            r = t - 4
            copy("do", r).wait_recv()
            copy("ds", r).wait_recv()
            mix(r)

        @pl.when(within(t - 4) & hub)
        def _():
            copy("y1", t - 4).start()
            copy("t0", t - 4).start()

        @pl.when(within(t - 4) & helper)
        def _():
            copy("yx", t - 4).start()

        @pl.when(within(t))
        def _():
            copy("b1", t).wait_recv()
            copy("r3", t).start()
            copy("b3", t).wait_recv()
            copy("r1", t).start()

        @pl.when(within(t + 2))
        def _():
            x_start(t + 2)

        @pl.when(t == 0)
        def _():
            cload.wait()
            prefix[:, 0] = jnp.zeros((tiles, 16, n), F32)
            right[:, nq * height:] = jnp.zeros((pair_k, right.shape[1] - nq * height, n), BF)
            lane = lax.broadcasted_iota(jnp.int32, (n, 128), 1) < height

            @pl.loop(0, (nq + 1) // 2)
            def _(h):
                for d in range(n // 128):
                    lhs = cmat[2 * h, :, d * 128:(d + 1) * 128].astype(F32)
                    rhs = cmat[jnp.minimum(2 * h + 1, nq - 1), :, d * 128:(d + 1) * 128].astype(F32)
                    rhs = jnp.where(2 * h + 1 < nq, rhs, jnp.zeros_like(rhs))
                    to = pl.ds(pl.multiple_of(h * 128, 128), 128)
                    cst[2 * d, :, to] = jnp.where(lane, lhs, pltpu.roll(rhs, height, 1)).astype(BF)
                    cst[2 * d + 1, :, to] = jnp.where(lane, pltpu.roll(lhs, height, 1), rhs).astype(BF)

        @pl.when(t == 1)
        def _():
            sort_tables()

        @pl.when(within(t - 1))
        def _():
            r = t - 1
            copy("a3", r).wait_recv()
            copy("r3", r).wait_recv()
            copy("r1", r).wait_recv()
            copy("z", r).start()
            copy("a1", r).wait_recv()
            copy("do", r).start()

        @pl.when(within(t - 3))
        def _():
            r = t - 3
            copy("z", r).wait_recv()
            copy("ds", r).start()

        @pl.when(within(t - 7))
        def _():
            r = t - 7

            @pl.when(helper)
            def _():
                for name in ("t0", "t2", "t1", "t3"):
                    copy(name, r).wait_recv()

            @pl.when(r % SUB == SUB - 1)
            def _():
                take(r // SUB)

            @pl.when(r == SUB - 1)
            def _():
                classes0()

            @pl.when((r % SUB == SUB - 1) & (r >= SUB))
            def _():
                classes(r // SUB, 0)
                classes(r // SUB, own_k)

        @pl.when(within(t - 8) & ((t - 8) % SUB == SUB - 1))
        def _():
            rights()

        @pl.when(within(t - 5) & hub)
        def _():
            r = t - 5
            copy("yx", r).wait_recv()
            copy("yf", r).start()
            copy("t2", r).start()

        @pl.when(within(t - 6) & hub)
        def _():
            r = t - 6
            copy("y1", r).wait_recv()
            copy("t1", r).start()
            copy("yf", r).wait_recv()
            copy("t3", r).start()

    finish()

    for name, ref in (("a1", a), ("a3", a), ("r1", rc), ("r3", rp), ("z", far.at[0]), ("ds", ps)):
        all_sent(name, ref)

    @pl.when(hub)
    def _():
        for name in ("y1", "yf", "t0", "t1", "t2", "t3"):
            all_sent(name, ps)

    @pl.when(helper)
    def _():
        all_sent("yx", ps)

    for k in range(pair_k):
        mine_too = hub & ((k // own_k) == xl)

        @pl.when(mine_too)
        def _():
            keep(k).wait()

        @pl.when(jnp.logical_not(mine_too))
        def _():
            osend(k, pair).wait_send()
    for p in range(2):
        for j in range(own_k):
            @pl.when(helper | (p != xl))
            def _():
                pltpu.make_async_copy(out.at[j, p], out.at[j, p], orecv_sem.at[p * own_k + j]).wait()


def body(green_blocks, transfer_index, photon_shift, photon_occupancy, coupling):
    own_k, n = green_blocks.shape[0], green_blocks.shape[3]
    momenta, nq = transfer_index.shape[1], coupling.shape[0]
    pair_k = 2 * own_k
    chunks, height = n // ROWS, ROWS * SUB
    deep = (nq + 1) // 2 * 2 * height
    count = lax.axis_size("en")
    smem = pl.BlockSpec(memory_space=pltpu.SMEM)
    hbm = pl.BlockSpec(memory_space=pl.ANY)
    dma = pltpu.SemaphoreType.DMA
    parts = pl.pallas_call(
        functools.partial(kernel, n, nq, own_k, count),
        out_shape=jax.ShapeDtypeStruct((own_k, 2, chunks, ROWS, n), BF),
        in_specs=[pl.BlockSpec(memory_space=pltpu.VMEM), smem, smem, hbm, hbm],
        out_specs=hbm,
        scratch_shapes=[
            pltpu.VMEM((own_k, 2, n, n), F32),
            pltpu.VMEM((chunks, own_k, ROWS, n), BF),
            pltpu.VMEM((chunks, pair_k, ROWS, n), BF),
            pltpu.VMEM((2, chunks, pair_k, ROWS, n), BF),
            pltpu.VMEM((chunks, own_k, ROWS, n // 2), BF),
            pltpu.VMEM((chunks, own_k, ROWS, n // 2), BF),
            pltpu.VMEM((chunks, pair_k, ROWS, n), BF),
            pltpu.VMEM((chunks, pair_k, ROWS, n), BF),
            pltpu.VMEM((chunks, momenta + pair_k, ROWS, n), BF),
            pltpu.VMEM((nq, n, n), BF),
            pltpu.VMEM((n // height, n, deep), BF),
            pltpu.VMEM((momenta, height, n), BF),
            pltpu.VMEM((height // 16, momenta + 1, 16, n), F32),
            pltpu.VMEM((nq, pair_k * height, n), BF),
            pltpu.VMEM((pair_k, deep, n), BF),
            pltpu.VMEM((8, 128), jnp.int32),
            pltpu.VMEM((4, 8, 128), jnp.int32),
            pltpu.VMEM((4, 8, 128), jnp.int32),
            pltpu.SMEM((2, 8, 128), jnp.int32),
            pltpu.SMEM((2, 8, 128), jnp.int32),
            pltpu.SMEM((2, 8, 128), jnp.int32),
            dma((chunks,)), dma(()), dma((len(RELAYED),)), dma((len(RELAYED), chunks)),
            dma((pair_k,)), dma((pair_k,)), dma((3,)), dma((3,)), dma((3,)),
        ],
        compiler_params=pltpu.CompilerParams(
            collective_id=0, has_side_effects=True, vmem_limit_bytes=67_043_328),
        name="scba",
    )(transfer_index, photon_shift, photon_occupancy, green_blocks, coupling)
    return parts.reshape(green_blocks.shape).astype(F32)


def solution(mesh):
    placed = (P("mom", "en", None, None, None), P("mom", None), P("mom"), P(), P())
    return jax.shard_map(
        body,
        mesh=mesh,
        in_specs=placed,
        out_specs=P("mom", "en", None, None, None),
        check_vma=False,
    )
```
